128 devices in a mesh: dp: 128 (over z, y, x, core).
Axes of the slice: x: 4, y: 4, z: 4, core: 2. Of those that a mesh axis runs over, the one named last changes fastest.
Arguments:
- hidden: bfloat16 [65536, 4096], P('dp')
- router_w: bfloat16 [4096, 128], replicated
- expert_idx: int32 [65536, 8], P('dp')
- gate_grad: float32 [65536, 8], P('dp')
Outputs:
- output 1: float32 [65536, 8], P('dp')
- output 2: float32 [], replicated
- output 3: bfloat16 [65536, 4096], P('dp')
- output 4: float32 [4096, 128], replicated
All inputs are finite; a program needn't handle non-finite values.
Results may differ from the reference program's by a relative error of at most 0.00786606.
Values sent between devices are 32-bit elements.
A program may use at most 1 GiB of HBM per device.

```python
import jax
import jax.numpy as jnp
from jax import lax

TOKENS = 65536
HIDDEN = 4096
EXPERTS = 128
TOP_K = 8
SHARDS = 128
ALPHA = 0.001
ROWS_PER_SHARD = TOKENS // SHARDS
LOSS_SCALE = float(TOKENS * EXPERTS * EXPERTS)


def draw_routes(key):
    key_bias, key_noise, key_shift = jax.random.split(key, 3)
    shard_bias = jax.random.randint(key_bias, (SHARDS, EXPERTS), 0, 48)
    row_noise = jax.random.randint(key_noise, (TOKENS, EXPERTS), 0, 32)
    row_shift = jax.random.randint(key_shift, (SHARDS, 1), 0, EXPERTS)
    row_pos = jnp.arange(ROWS_PER_SHARD)[None, :] + row_shift
    forced = (row_pos % EXPERTS).reshape(TOKENS, 1)
    expert_ids = jnp.arange(EXPERTS)[None, :]
    scores = jnp.repeat(shard_bias, ROWS_PER_SHARD, axis=0) + row_noise + 1000 * (expert_ids == forced).astype(jnp.int32)
    scores = scores * EXPERTS + expert_ids
    chosen = lax.top_k(scores, TOP_K)[1]
    return chosen.astype(jnp.int32)


def setup_inputs(seed: int = 0) -> dict:
    keys = jax.random.split(jax.random.key(seed), 5)
    shard_mean = 0.5 * jax.random.normal(keys[0], (SHARDS, HIDDEN), jnp.float32)
    hidden = jax.random.normal(keys[1], (TOKENS, HIDDEN), jnp.float32) + jnp.repeat(shard_mean, ROWS_PER_SHARD, axis=0)
    router_w = jax.random.normal(keys[2], (HIDDEN, EXPERTS), jnp.float32) * HIDDEN ** -0.5
    expert_idx = draw_routes(keys[3])
    grad_scale = ALPHA * TOP_K * TOP_K / (TOKENS * EXPERTS)
    gate_grad = jax.random.normal(keys[4], (TOKENS, TOP_K), jnp.float32) * grad_scale
    return {"hidden": hidden.astype(jnp.bfloat16), "router_w": router_w.astype(jnp.bfloat16), "expert_idx": expert_idx, "gate_grad": gate_grad}


def reference(hidden, router_w, expert_idx, gate_grad):
    logits = jnp.dot(hidden, router_w, preferred_element_type=jnp.float32)
    expert_freq = jnp.bincount(expert_idx.reshape(-1), length=EXPERTS).astype(jnp.float32) / TOKENS

    def objective(logit_vals):
        router_probs = jax.nn.softmax(logit_vals, axis=-1)
        picked = jnp.take_along_axis(router_probs, expert_idx, axis=1)
        gate_probs = picked / jnp.sum(picked, axis=1, keepdims=True)
        aux_loss = ALPHA * EXPERTS * jnp.sum(expert_freq * jnp.mean(router_probs, axis=0))
        return gate_probs, aux_loss

    (gate_probs, aux_loss), pullback = jax.vjp(objective, logits)
    logit_grad = pullback((LOSS_SCALE * gate_grad, jnp.asarray(LOSS_SCALE, jnp.float32)))[0]
    grad_bf = logit_grad.astype(jnp.bfloat16)
    hidden_grad = jnp.dot(grad_bf, router_w.T, preferred_element_type=jnp.float32).astype(jnp.bfloat16)
    router_grad = jnp.dot(hidden.T, grad_bf, preferred_element_type=jnp.float32)
    return gate_probs, aux_loss, hidden_grad, router_grad
```

```python
import jax
import jax.numpy as jnp
from jax import lax
from jax.experimental import pallas as pl
from jax.experimental.pallas import tpu as pltpu
from jax.sharding import PartitionSpec as P

LOSS_ALPHA = 0.001
MESH = pl.DeviceIdType.MESH
AXIS = "dp"
RING = 4
STRIDES = (2, 8, 32)
REGIONS = ((0, 768), (768, 640), (1408, 640))
CHUNKS = 4
F32 = jnp.float32
BF16 = jnp.bfloat16


def peers_of(me, stride):
    pos = lax.rem(me // stride, RING)
    out = []
    for r in (1, 2, 3):
        q = lax.rem(pos + r, RING)
        out.append((me + (q - pos) * stride, q))
    return pos, out


def make_kernel(tokens, width, experts, top_k, total_rows, loss_scale):
    half = width // 2
    kc = width // CHUNKS
    aux_scale = LOSS_ALPHA * experts / total_rows
    aux_coef = loss_scale * LOSS_ALPHA * experts / total_rows

    def kernel(hid_hbm, w_hbm, idx_hbm, gg_hbm, gate_ref, aux_ref, hg_ref, rg_ref,
               hid, w, idx, gg, probs, base, own, give, take, cnt, cnt_in, aux, aux_in,
               r1a, r1b, r1c, r2a, r2b, r2c, r3a, r3b, r3c, s1a, s1b, s1c, s2a, s2b, s2c,
               load_sem, send_sem, recv_sem):
        me = lax.axis_index(AXIS)
        core = lax.rem(me, 2)
        partner = me + 1 - 2 * core
        used = [0]
        sends = []

        def remote(src, dst, peer):
            n = used[0]
            used[0] += 1
            cp = pltpu.make_async_remote_copy(
                src_ref=src, dst_ref=dst, send_sem=send_sem.at[n], recv_sem=recv_sem.at[n],
                device_id=(peer,), device_id_type=MESH)
            sends.append(cp)
            return cp

        loads = [pltpu.make_async_copy(idx_hbm, idx, load_sem.at[0]),
                 pltpu.make_async_copy(gg_hbm, gg, load_sem.at[1])]
        for i in range(CHUNKS):
            loads.append(pltpu.make_async_copy(w_hbm.at[pl.ds(i * kc, kc)], w.at[pl.ds(i * kc, kc)], load_sem.at[2 + 2 * i]))
            loads.append(pltpu.make_async_copy(hid_hbm.at[:, pl.ds(i * kc, kc)], hid.at[:, pl.ds(i * kc, kc)], load_sem.at[3 + 2 * i]))
        for cp in loads:
            cp.start()

        barrier = pltpu.get_barrier_semaphore()
        greet = [partner]
        for stride in STRIDES:
            greet += [peer for peer, _ in peers_of(me, stride)[1]]
        for peer in greet:
            pl.semaphore_signal(barrier, inc=1, device_id=(peer,), device_id_type=MESH)

        loads[0].wait()
        expert = lax.broadcasted_iota(jnp.int32, (experts, tokens), 0)
        hits = jnp.zeros((experts, tokens), F32)
        for j in range(top_k):
            hits = hits + jnp.where(expert == idx[j:j + 1, :], 1.0, 0.0)
        cnt[0] = lax.dot_general(jnp.ones((8, tokens), BF16), hits.astype(BF16),
                                 (((1,), (1,)), ((), ())), preferred_element_type=F32)
        pl.semaphore_wait(barrier, len(greet))

        def tile_start(src, dst, level):
            if level == 0:
                cps = [remote(src.at[0], dst.at[0], partner)]
            else:
                cps = [remote(src.at[level], dst.at[3 * level - 2 + 2 - r], peer)
                       for r, (peer, _) in enumerate(peers_of(me, STRIDES[level - 1])[1])]
            for cp in cps:
                cp.start()
            return cps

        def tile_finish(src, dst, level, cps):
            for cp in cps:
                cp.wait_recv()
            if level == 0:
                return src[0] + dst[0]
            b = 3 * level - 2
            return (src[level] + dst[b + 1]) + (dst[b] + dst[b + 2])

        flight = tile_start(cnt, cnt_in, 0)
        logits = jnp.zeros((tokens, experts), F32)
        for i in range(CHUNKS):
            loads[2 + 2 * i].wait()
            loads[3 + 2 * i].wait()
            logits = logits + jnp.dot(hid[:, i * kc:(i + 1) * kc], w[i * kc:(i + 1) * kc, :], preferred_element_type=F32)
            if i < 3:
                cnt[i + 1] = tile_finish(cnt, cnt_in, i, flight)
                flight = tile_start(cnt, cnt_in, i + 1)

        lt = logits.T
        e = jnp.exp(lt - jnp.max(lt, axis=0, keepdims=True))
        p = e * (1.0 / jnp.sum(e, axis=0, keepdims=True))
        probs[...] = p
        picked = jnp.concatenate(
            [jnp.sum(jnp.where(expert == idx[j:j + 1, :], p, 0.0), axis=0, keepdims=True) for j in range(top_k)], axis=0)
        inv_sum = 1.0 / jnp.sum(picked, axis=0, keepdims=True)
        gate = picked * inv_sum
        gate_ref[...] = gate
        loads[1].wait()
        sg = loss_scale * gg[...]
        pick_grad = (sg - jnp.sum(sg * gate, axis=0, keepdims=True)) * inv_sum
        pg = jnp.zeros((experts, tokens), F32)
        for j in range(top_k):
            pg = pg + jnp.where(expert == idx[j:j + 1, :], pick_grad[j:j + 1, :], 0.0)
        base[...] = pg

        total = tile_finish(cnt, cnt_in, 3, flight)
        freq = jnp.broadcast_to(total[0:1, :], (experts, experts)).T * (1.0 / total_rows)
        freq = jnp.concatenate([freq] * (tokens // experts), axis=1)
        p = probs[...]
        pf = jnp.sum(p * freq, axis=0, keepdims=True)
        pg = base[...] + aux_coef * freq
        lg = p * (pg - jnp.sum(p * pg, axis=0, keepdims=True))
        gt = lg.astype(BF16)
        aux[0] = jnp.broadcast_to(sum(pf[:, i * 128:(i + 1) * 128] for i in range(tokens // 128)), (8, 128))
        aux_flight = tile_start(aux, aux_in, 0)

        away = pl.multiple_of((1 - core) * half, 128)
        mine = pl.multiple_of(core * half, 128)
        d2d = []
        for lo, n in REGIONS:
            part = jnp.dot(gt, hid[:, pl.ds(pl.multiple_of(away + lo, 128), n)], preferred_element_type=F32)
            give[pl.ds(lo, n)] = part.T
            cp = remote(give.at[pl.ds(lo, n)], take.at[pl.ds(lo, n)], partner)
            cp.start()
            d2d.append(cp)

        r1, r2, r3 = (r1a, r1b, r1c), (r2a, r2b, r2c), (r3a, r3b, r3c)
        s1, s2 = (s1a, s1b, s1c), (s2a, s2b, s2c)

        def order(k):
            out = []
            for level in range(3):
                a, b = STRIDES[(k + level) % 3], STRIDES[(k + level + 1) % 3]
                out.append(a * (1 - core) + b * core)
            return out

        plan = []
        for k, (lo, n) in enumerate(REGIONS):
            strides = order(k)
            plan.append((lo, n // 4, n // 16) + tuple(peers_of(me, s) for s in strides))

        rs1 = []
        for k, (lo, n) in enumerate(REGIONS):
            part = jnp.dot(gt, hid[:, pl.ds(pl.multiple_of(mine + lo, 128), n)], preferred_element_type=F32)
            d2d[k].wait_recv()
            own[pl.ds(lo, n)] = part.T + take[pl.ds(lo, n)]
            _, c1, c2, (pos1, peers1), _, _ = plan[k]
            cps = []
            for r, (peer, q) in enumerate(peers1):
                cp = remote(own.at[pl.ds(pl.multiple_of(lo + q * c1, 8), c1)], r1[k].at[2 - r], peer)
                cp.start()
                cps.append(cp)
            rs1.append(cps)
        aux[1] = tile_finish(aux, aux_in, 0, aux_flight)
        aux_flight = tile_start(aux, aux_in, 1)

        g = lg.T.astype(BF16)
        for i in range(CHUNKS):
            hg_ref[:, i * kc:(i + 1) * kc] = lax.dot_general(
                g, w[i * kc:(i + 1) * kc, :], (((1,), (1,)), ((), ())), preferred_element_type=F32).astype(BF16)

        rs2 = []
        for k in range(3):
            lo, c1, c2, (pos1, peers1), (pos2, peers2), _ = plan[k]
            for cp in rs1[k]:
                cp.wait_recv()
            s1[k][...] = (own[pl.ds(pl.multiple_of(lo + pos1 * c1, 8), c1)] + r1[k][1]) + (r1[k][0] + r1[k][2])
            cps = []
            for r, (peer, q) in enumerate(peers2):
                cp = remote(s1[k].at[pl.ds(pl.multiple_of(q * c2, 8), c2)], r2[k].at[2 - r], peer)
                cp.start()
                cps.append(cp)
            rs2.append(cps)
        aux[2] = tile_finish(aux, aux_in, 1, aux_flight)
        aux_flight = tile_start(aux, aux_in, 2)

        b3 = []
        for k in range(3):
            lo, c1, c2, _, (pos2, _), (_, peers3) = plan[k]
            for cp in rs2[k]:
                cp.wait_recv()
            s2[k][...] = (s1[k][pl.ds(pl.multiple_of(pos2 * c2, 8), c2)] + r2[k][1]) + (r2[k][0] + r2[k][2])
            cps = []
            for r, (peer, q) in enumerate(peers3):
                cp = remote(s2[k], r3[k].at[2 - r], peer)
                cp.start()
                cps.append(cp)
            b3.append(cps)
        aux[3] = tile_finish(aux, aux_in, 2, aux_flight)
        aux_flight = tile_start(aux, aux_in, 3)

        ag2 = []
        for k in range(3):
            lo, c1, c2, (pos1, _), (pos2, peers2), _ = plan[k]
            for cp in b3[k]:
                cp.wait_recv()
            at = pl.ds(pl.multiple_of(mine + lo + pos1 * c1 + pos2 * c2, 8), c2)
            rg_ref[at] = (s2[k][...] + r3[k][1]) + (r3[k][0] + r3[k][2])
            cps = []
            for peer, q in peers2:
                cp = remote(rg_ref.at[at], rg_ref.at[at], peer)
                cp.start()
                cps.append(cp)
            ag2.append(cps)
        total_aux = tile_finish(aux, aux_in, 3, aux_flight)
        aux_ref[...] = jnp.broadcast_to(aux_scale * jnp.sum(total_aux[0:1, :], axis=1, keepdims=True), (8, 128))

        ag1, back = [], []
        for k in range(3):
            lo, c1, c2, (pos1, peers1), _, _ = plan[k]
            for cp in ag2[k]:
                cp.wait_recv()
            at = pl.ds(pl.multiple_of(mine + lo + pos1 * c1, 8), c1)
            cps = []
            for peer, q in peers1:
                cp = remote(rg_ref.at[at], rg_ref.at[at], peer)
                cp.start()
                cps.append(cp)
            ag1.append(cps)
            cp = remote(rg_ref.at[at], rg_ref.at[at], partner)
            cp.start()
            back.append(cp)
        for k in range(3):
            lo, c1, c2, (pos1, peers1), _, _ = plan[k]
            for r in range(3):
                ag1[k][r].wait_recv()
                q = lax.rem(pos1 + RING - (r + 1), RING)
                at = pl.ds(pl.multiple_of(mine + lo + q * c1, 8), c1)
                cp = remote(rg_ref.at[at], rg_ref.at[at], partner)
                cp.start()
                back.append(cp)
        for cp in back:
            cp.wait_recv()
        for cp in sends:
            cp.wait_send()

    return kernel


def solution(mesh):
    group_size = mesh.shape[AXIS]

    def device_step(hidden, router_w, expert_idx, gate_grad):
        tokens, width = hidden.shape
        experts, top_k = router_w.shape[1], expert_idx.shape[1]
        total_rows = tokens * group_size
        loss_scale = float(total_rows * experts * experts)
        half = width // 2
        vmem = pl.BlockSpec(memory_space=pltpu.VMEM)
        hbm = pl.BlockSpec(memory_space=pltpu.HBM)
        n_sems = 100
        scratch = [
            pltpu.VMEM((tokens, width), BF16), pltpu.VMEM((width, experts), BF16),
            pltpu.VMEM((top_k, tokens), jnp.int32), pltpu.VMEM((top_k, tokens), F32),
            pltpu.VMEM((experts, tokens), F32), pltpu.VMEM((experts, tokens), F32),
            pltpu.VMEM((half, experts), F32), pltpu.VMEM((half, experts), F32), pltpu.VMEM((half, experts), F32),
            pltpu.VMEM((4, 8, 128), F32), pltpu.VMEM((10, 8, 128), F32),
            pltpu.VMEM((4, 8, 128), F32), pltpu.VMEM((10, 8, 128), F32),
        ]
        scratch += [pltpu.VMEM((3, n // 4, experts), F32) for _, n in REGIONS]
        scratch += [pltpu.VMEM((3, n // 16, experts), F32) for _, n in REGIONS]
        scratch += [pltpu.VMEM((3, n // 16, experts), F32) for _, n in REGIONS]
        scratch += [pltpu.VMEM((n // 4, experts), F32) for _, n in REGIONS]
        scratch += [pltpu.VMEM((n // 16, experts), F32) for _, n in REGIONS]
        scratch += [pltpu.SemaphoreType.DMA((2 + 2 * CHUNKS,)), pltpu.SemaphoreType.DMA((n_sems,)), pltpu.SemaphoreType.DMA((n_sems,))]
        gate, aux, hg, rg = pl.pallas_call(
            make_kernel(tokens, width, experts, top_k, total_rows, loss_scale),
            out_shape=(jax.ShapeDtypeStruct((top_k, tokens), F32), jax.ShapeDtypeStruct((8, 128), F32),
                       jax.ShapeDtypeStruct((tokens, width), BF16), jax.ShapeDtypeStruct((width, experts), F32)),
            in_specs=[hbm, hbm, hbm, hbm],
            out_specs=(vmem, vmem, vmem, vmem),
            scratch_shapes=scratch,
            compiler_params=pltpu.CompilerParams(collective_id=0, has_side_effects=True, vmem_limit_bytes=40 * 1024 * 1024),
            name="router",
        )(*[pltpu.with_memory_space_constraint(x, pltpu.HBM) for x in (hidden, router_w, expert_idx.T, gate_grad.T)])
        return gate.T, aux[0, 0], hg, rg

    return jax.shard_map(device_step, mesh=mesh, in_specs=(P("dp", None), P(None, None), P("dp", None), P("dp", None)), out_specs=(P("dp", None), P(), P("dp", None), P(None, None)), check_vma=False)
```
